256 devices in a mesh: tm: 16 (over x_hi, y, core), space: 16 (over x_lo, z).
Axes of the slice: x: 4 (x_hi: 2, x_lo: 2; x = x_hi * 2 + x_lo), y: 4, z: 8, core: 2. Of those that a mesh axis runs over, the one named last changes fastest.
Arguments:
- gauge_links: float32 [16, 2, 3, 3, 3, 32, 1024], P('tm', None, None, None, None, 'space'), may hold values from -1 to 1, as said below
- time_links: float32 [16, 2, 3, 3, 32, 1024], P('tm', None, None, None, 'space'), may hold values from -1 to 1, as said below
- sink_vectors: bfloat16 [16, 2, 128, 3, 32, 1024], P('tm', None, None, None, 'space'), may hold values from -0.29882812 to 0.29882812
- source_times: int32 [4], replicated, may hold values from 0 to 15
- source_index: int32 [4, 2], replicated, may hold values from 0 to 127
- kinetic_coef: float32 [4, 2], replicated, may hold values from 0.005 to 0.12
Outputs:
- perambulator: float32 [2, 4, 2, 16, 128], P(None, None, None, 'tm', 'space')
The draws below stay inside these ranges and needn't reach their ends.
Inputs may be any that keep to these rules, and one draw needn't show every extreme that they name: `gauge_links`: each link is a special unitary 3 x 3 matrix. `time_links`: each link is a special unitary 3 x 3 matrix.
All inputs are finite; a program needn't handle non-finite values.
Results may differ from the reference program's by a relative error of at most 0.0029.
Values may be sent and summed in bfloat16 or wider, within the bound.
A program may use at most 128 MiB of HBM per device.

```python
import math
from functools import partial
import jax
import jax.numpy as jnp
from jax import lax

LS = 32
NEV = 128
SRC = 2
NSRCT = 4
NT = 16
LX = 32


def special_unitary(key, lead):
    keys = jax.random.split(key, 4)
    first = jax.random.normal(keys[0], lead + (3,), jnp.float32) + 1j * jax.random.normal(keys[1], lead + (3,), jnp.float32)
    second = jax.random.normal(keys[2], lead + (3,), jnp.float32) + 1j * jax.random.normal(keys[3], lead + (3,), jnp.float32)
    first = first / jnp.sqrt(jnp.sum(jnp.real(first) * jnp.real(first) + jnp.imag(first) * jnp.imag(first), axis=-1, keepdims=True))
    second = second - jnp.sum(jnp.conj(first) * second, axis=-1, keepdims=True) * first
    second = second / jnp.sqrt(jnp.sum(jnp.real(second) * jnp.real(second) + jnp.imag(second) * jnp.imag(second), axis=-1, keepdims=True))
    third = jnp.conj(jnp.cross(first, second))
    matrix = jnp.stack([first, second, third], axis=-2)
    return jnp.stack([jnp.real(matrix), jnp.imag(matrix)], axis=0).astype(jnp.float32)


def draw_gauge_links(key, part):
    matrices = special_unitary(jax.random.fold_in(key, 11), (NT, 3, LX, LS * LS))
    return matrices.transpose(1, 0, 2, 5, 6, 3, 4)


def draw_time_links(key, part):
    matrices = special_unitary(jax.random.fold_in(key, 23), (NT, LX, LS * LS))
    return matrices.transpose(1, 0, 4, 5, 2, 3)


def with_ends(result, own_key, smallest, top_value):
    place = [jax.random.randint(jax.random.fold_in(own_key, axis), (), 0, length) for axis, length in enumerate(result.shape)]
    widest = result.shape.index(max(result.shape))
    neighbour = place[:widest] + [(place[widest] + 1) % result.shape[widest]] + place[widest + 1:]
    return result.at[tuple(place)].set(smallest).at[tuple(neighbour)].set(top_value)


def levels(key, shape, pieces, least, top_value):
    gain, own = 1.0, jax.random.fold_in(key, 6)
    for dim, shards_of in pieces:
        steps = jnp.exp(jax.random.uniform(jax.random.fold_in(own, dim), (shards_of,), jnp.float32, least / len(pieces), top_value / len(pieces)))
        gain = gain * jnp.repeat(steps, shape[dim] // shards_of).reshape([-1 if axis == dim else 1 for axis in range(len(shape))])
    return gain


def scatter_about(stream_key, dims, deviation, most, shards=(), dtype=jnp.bfloat16):
    values = jax.random.normal(stream_key, dims, jnp.float32) * deviation
    if len(shards) > 0:
        values = levels(stream_key, dims, shards, -0.22, 0.18) * values
    return jnp.clip(values, min=-most, max=most).astype(dtype)


def setup_inputs(seed: int = 0) -> dict:
    streams_of = jax.random.split(jax.random.key(seed), 7)
    gauge_links = draw_gauge_links(jax.random.fold_in(streams_of[6], 71), 0)
    time_links = draw_time_links(jax.random.fold_in(streams_of[6], 71), 0)
    sink_vectors = scatter_about(streams_of[2], (NT, 2, NEV, 3, LX, LS * LS), 0.05, 0.29882812, ((0, 16), (4, 16)))
    source_times = with_ends(jax.random.randint(streams_of[3], (NSRCT,), 0, NT), jax.random.fold_in(streams_of[3], 1), 0, NT - 1).astype(jnp.int32)
    source_index = with_ends(jax.random.randint(streams_of[4], (NSRCT, SRC), 0, NEV), jax.random.fold_in(streams_of[4], 1), 0, NEV - 1).astype(jnp.int32)
    kinetic_coef = jnp.clip(jnp.exp(jax.random.uniform(streams_of[5], (NSRCT, SRC), jnp.float32, math.log(0.005), math.log(0.12))), 0.005, 0.12)
    return dict(gauge_links=gauge_links, time_links=time_links, sink_vectors=sink_vectors, source_times=source_times, source_index=source_index, kinetic_coef=kinetic_coef)


einsum_high = partial(jnp.einsum, precision=lax.Precision.HIGHEST)


def colour_apply(matrix, vector_in):
    real_part = einsum_high('abxs,bvxs->avxs', matrix[0], vector_in[0]) - einsum_high('abxs,bvxs->avxs', matrix[1], vector_in[1])
    imag_part = einsum_high('abxs,bvxs->avxs', matrix[0], vector_in[1]) + einsum_high('abxs,bvxs->avxs', matrix[1], vector_in[0])
    return jnp.stack([real_part, imag_part])


def colour_adjoint(matrix, vector_in):
    real_part = einsum_high('baxs,bvxs->avxs', matrix[0], vector_in[0]) + einsum_high('baxs,bvxs->avxs', matrix[1], vector_in[1])
    imag_part = einsum_high('baxs,bvxs->avxs', matrix[0], vector_in[1]) - einsum_high('baxs,bvxs->avxs', matrix[1], vector_in[0])
    return jnp.stack([real_part, imag_part])


def shift_up(values, direction):
    if direction == 0:
        return jnp.roll(values, -1, axis=3)
    if direction == 1:
        return jnp.roll(values, -LS, axis=-1)
    z_index = jnp.arange(values.shape[-1]) % LS
    return jnp.where(z_index == LS - 1, jnp.roll(values, LS - 1, axis=-1), jnp.roll(values, -1, axis=-1))


def shift_down(values, direction):
    if direction == 0:
        return jnp.roll(values, 1, axis=3)
    if direction == 1:
        return jnp.roll(values, LS, axis=-1)
    z_index = jnp.arange(values.shape[-1]) % LS
    return jnp.where(z_index == 0, jnp.roll(values, -(LS - 1), axis=-1), jnp.roll(values, 1, axis=-1))


def laplace_full(wavefn, slice_links):
    summed = -6.0 * wavefn
    for direction in range(3):
        matrix = slice_links[:, direction]
        summed = summed + colour_apply(matrix, shift_up(wavefn, direction))
        summed = summed + colour_adjoint(shift_down(matrix, direction), shift_down(wavefn, direction))
    return summed


def project_slice(sink_slice, evolved):
    rounded = evolved.astype(jnp.bfloat16).astype(jnp.float32)
    sinks = sink_slice.astype(jnp.float32)
    real_part = jnp.einsum('ecxs,cvxs->ve', sinks[0], rounded[0]) + jnp.einsum('ecxs,cvxs->ve', sinks[1], rounded[1])
    imag_part = jnp.einsum('ecxs,cvxs->ve', sinks[0], rounded[1]) - jnp.einsum('ecxs,cvxs->ve', sinks[1], rounded[0])
    return jnp.stack([real_part, imag_part])


def reference(gauge_links, time_links, sink_vectors, source_times, source_index, kinetic_coef):
    per_time = []
    for which in range(NSRCT):
        start = source_times[which].astype(jnp.int32)
        start_sinks = lax.dynamic_index_in_dim(sink_vectors, start, 0, keepdims=False)
        source = jnp.take(start_sinks, source_index[which], axis=1).astype(jnp.float32).transpose(0, 2, 1, 3, 4)
        weight = (0.5 * kinetic_coef[which]).astype(jnp.float32)[None, None, :, None, None]

        def advance_slice(rounds, state_pair):
            wavefn, correlation_table = state_pair
            slice_no = ((start + rounds) % NT).astype(jnp.int32)
            slice_links = lax.dynamic_index_in_dim(gauge_links, slice_no, 0, keepdims=False)
            time_link = lax.dynamic_index_in_dim(time_links, slice_no, 0, keepdims=False)
            sink_slice = lax.dynamic_index_in_dim(sink_vectors, slice_no, 0, keepdims=False)
            halfway = wavefn + weight * laplace_full(wavefn, slice_links)
            turned = colour_adjoint(time_link, halfway)
            evolved = turned + weight * laplace_full(turned, slice_links)
            correlations = project_slice(sink_slice, evolved)
            zero = jnp.zeros((), jnp.int32)
            correlation_table = lax.dynamic_update_slice(correlation_table, correlations[:, :, None, :], (zero, zero, slice_no, zero))
            return evolved, correlation_table

        empty = jnp.zeros((2, SRC, NT, NEV), jnp.float32)
        _, correlation_table = lax.fori_loop(0, NT, advance_slice, (source, empty))
        per_time.append(correlation_table)
    return jnp.stack(per_time, axis=1)
```

```python
import functools

import jax
import jax.numpy as jnp
from jax import lax
from jax.experimental import pallas as pl
from jax.experimental.pallas import tpu as pltpu
from jax.sharding import PartitionSpec as P

MESH = pl.DeviceIdType.MESH
F32 = jnp.float32
BF16 = jnp.bfloat16
SLOTS = 4


def modulo(value, length):
    return jnp.where(value < 0, value + length, value)


def times(links, field):
    real, imag = None, None
    for b in range(3):
        u_re, u_im = links(0, slice(None), b), links(1, slice(None), b)
        f_re, f_im = field[0][b : b + 1], field[1][b : b + 1]
        re = u_re * f_re - u_im * f_im
        im = u_re * f_im + u_im * f_re
        real, imag = (re, im) if real is None else (real + re, imag + im)
    return real, imag


def adjoint_times(links, field):
    real, imag = None, None
    for b in range(3):
        u_re, u_im = links(0, b, slice(None)), links(1, b, slice(None))
        f_re, f_im = field[0][b : b + 1], field[1][b : b + 1]
        re = u_re * f_re + u_im * f_im
        im = u_re * f_im - u_im * f_re
        real, imag = (re, im) if real is None else (real + re, imag + im)
    return real, imag


def kernel(
    n_tm, n_space, rounds,
    times_ref, index_ref, coef_ref, gauge_hbm, temporal_hbm, sinks_hbm,
    out_ref,
    gauge_in, temporal_in, sinks, link_x, link_yz, link_t,
    up_out, down_out, low_links, high_links,
    staged, own_src, low_src, high_src,
    recv_own, recv_low, recv_high, sent_own, record,
    field, turned, chosen, summed, partial, parts,
    local_sem, halo_send, halo_recv, step_send, step_recv, part_send, part_recv,
):
    t = lax.axis_index("tm")
    i = lax.axis_index("space")
    after, before = lax.rem(t + 1, n_tm), lax.rem(t + n_tm - 1, n_tm)
    above, below = lax.rem(i + 1, n_space), lax.rem(i + n_space - 1, n_space)

    fetches = [
        pltpu.make_async_copy(gauge_hbm, gauge_in, local_sem.at[0]),
        pltpu.make_async_copy(temporal_hbm, temporal_in, local_sem.at[1]),
        pltpu.make_async_copy(sinks_hbm, sinks, local_sem.at[2]),
    ]
    for fetch in fetches:
        fetch.start()

    barrier = pltpu.get_barrier_semaphore()
    for near_t in (before, after):
        for near_i in (below, i, above):
            pl.semaphore_signal(
                barrier, inc=1, device_id={"tm": near_t, "space": near_i}, device_id_type=MESH
            )
    for step in range(1, n_space):
        pl.semaphore_signal(
            barrier, inc=1,
            device_id={"tm": t, "space": lax.rem(i + step, n_space)}, device_id_type=MESH,
        )

    recv_own[0] = jnp.zeros_like(recv_own[0])
    recv_low[0] = jnp.zeros_like(recv_low[0])
    recv_high[0] = jnp.zeros_like(recv_high[0])

    start = [times_ref[k] for k in range(SLOTS)]
    late, lane = [], []
    for k in range(SLOTS):
        free = []
        for d in range(SLOTS - 1):
            place = modulo(start[k] - d, n_tm)
            ok = jnp.int32(1)
            for other in lane:
                ok = jnp.where(other == place, 0, ok)
            free.append(ok)
        d = jnp.int32(SLOTS - 1)
        for value in reversed(range(SLOTS - 1)):
            d = jnp.where(free[value] == 1, value, d)
        late.append(d)
        lane.append(modulo(start[k] - d, n_tm))
    here, which = [], []
    for d in range(SLOTS):
        count = jnp.int32(0)
        index = [jnp.int32(0), jnp.int32(0)]
        for k in range(SLOTS):
            match = jnp.where(start[k] == t, jnp.where(late[k] == d, 1, 0), 0)
            count = count + match
            index = [index[j] + match * index_ref[k, j] for j in range(2)]
        here.append(count)
        which.append(index)

    fetches[0].wait()
    fetches[1].wait()
    for x in range(2):
        for row in range(3):
            for col in range(3):
                for mu in range(3):
                    pair = []
                    for ri in range(2):
                        plane = gauge_in[ri, mu, row, col, pl.ds(x, 8, stride=2), :]
                        pair.append(plane)
                        if mu == 0:
                            link_x[2 + x, ri, row, col] = plane
                        else:
                            link_yz[1 + x, mu - 1, ri, row, col] = plane
                    packed = jnp.concatenate(pair, axis=0).astype(BF16)
                    if x == 1:
                        up_out[(mu * 3 + row) * 3 + col] = packed
                    else:
                        down_out[(mu * 3 + row) * 3 + col] = packed
                        if mu == 0:
                            up_out[36 + row * 3 + col] = packed
                pair = []
                for ri in range(2):
                    plane = temporal_in[ri, row, col, pl.ds(x, 8, stride=2), :]
                    pair.append(plane)
                    link_t[1 + x, ri, row, col] = plane
                packed = jnp.concatenate(pair, axis=0).astype(BF16)
                if x == 1:
                    up_out[27 + row * 3 + col] = packed
                else:
                    down_out[27 + row * 3 + col] = packed

    fetches[2].wait()
    for d in range(SLOTS):
        keep = here[d].astype(F32)
        for j in range(2):
            for ri in range(2):
                for c in range(3):
                    staged[d, j, ri * 3 + c] = sinks[ri, which[d][j], c].astype(F32) * keep
    for d in range(SLOTS):
        for j in range(2):
            for part in range(6):
                planes = [staged[d, j, part, pl.ds(x, 8, stride=2), :] for x in range(2)]
                own_src[d, j, part] = jnp.concatenate(planes, axis=0).astype(BF16)

    pl.semaphore_wait(barrier, 6 + n_space - 1)

    def halo(number, src, dst, device):
        return pltpu.make_async_remote_copy(
            src_ref=src, dst_ref=dst, send_sem=halo_send.at[number], recv_sem=halo_recv.at[number],
            device_id={"tm": t, "space": device}, device_id_type=MESH,
        )

    source_halos = [
        (
            halo(2 * d, own_src.at[d], low_src.at[d], above),
            halo(2 * d + 1, own_src.at[d], high_src.at[d], below),
        )
        for d in range(SLOTS)
    ]
    link_halos = (
        halo(2 * SLOTS, up_out, low_links, above),
        halo(2 * SLOTS + 1, down_out, high_links, below),
    )
    for copy in link_halos + source_halos[0] + source_halos[1] + source_halos[2] + source_halos[3]:
        copy.start()

    link_halos[0].wait_recv()
    for row in range(3):
        for col in range(3):
            for mu in range(3):
                both = low_links[(mu * 3 + row) * 3 + col].astype(F32)
                for ri in range(2):
                    if mu == 0:
                        link_x[1, ri, row, col] = both[8 * ri : 8 * ri + 8]
                    else:
                        link_yz[0, mu - 1, ri, row, col] = both[8 * ri : 8 * ri + 8]
            both = low_links[27 + row * 3 + col].astype(F32)
            for ri in range(2):
                link_t[0, ri, row, col] = both[8 * ri : 8 * ri + 8]
            both = low_links[36 + row * 3 + col].astype(F32)
            for ri in range(2):
                link_x[0, ri, row, col] = both[8 * ri : 8 * ri + 8]
    link_halos[1].wait_recv()
    for row in range(3):
        for col in range(3):
            for mu in range(3):
                both = high_links[(mu * 3 + row) * 3 + col].astype(F32)
                for ri in range(2):
                    if mu == 0:
                        link_x[4, ri, row, col] = both[8 * ri : 8 * ri + 8]
                    else:
                        link_yz[3, mu - 1, ri, row, col] = both[8 * ri : 8 * ri + 8]
            both = high_links[27 + row * 3 + col].astype(F32)
            for ri in range(2):
                link_t[3, ri, row, col] = both[8 * ri : 8 * ri + 8]

    lanes = lax.broadcasted_iota(jnp.int32, (3, 8, 128), 2)
    z = lax.rem(lanes, 32)
    first_z, last_z = z == 0, z == 31
    low_lanes, high_lanes = lanes < 32, lanes >= 96

    def up(values, direction):
        if direction == 0:
            moved = pltpu.roll(values, 96, 2)
            return jnp.where(high_lanes, pltpu.roll(moved, 7, 1), moved)
        return jnp.where(last_z, pltpu.roll(values, 31, 2), pltpu.roll(values, 127, 2))

    def down(values, direction):
        if direction == 0:
            moved = pltpu.roll(values, 32, 2)
            return jnp.where(low_lanes, pltpu.roll(moved, 1, 1), moved)
        return jnp.where(first_z, pltpu.roll(values, 97, 2), pltpu.roll(values, 1, 2))

    def relaxed(source, q, links_q, weight):
        at = lambda p: (source[p, 0:3], source[p, 3:6])
        centre = at(q)
        re, im = times(lambda ri, a, b: link_x[links_q + 1, ri, a, b], at(q + 1))
        more = adjoint_times(lambda ri, a, b: link_x[links_q, ri, a, b], at(q - 1))
        re, im = re + more[0], im + more[1]
        for direction in range(2):
            links = lambda ri, a, b: link_yz[links_q, direction, ri, a, b]
            more = times(links, tuple(up(part, direction) for part in centre))
            re, im = re + more[0], im + more[1]
            more = tuple(down(part, direction) for part in adjoint_times(links, centre))
            re, im = re + more[0], im + more[1]
        rest = 1.0 - 6.0 * weight
        return rest * centre[0] + weight * re, rest * centre[1] + weight * im

    def hop(number, device_t, r, j):
        if number == 0:
            src, dst, target = record.at[r, j], recv_low.at[r + 1, j], above
        elif number == 1:
            src, dst, target = record.at[r, j], recv_high.at[r + 1, j], below
        else:
            src, dst, target = sent_own.at[r, j], recv_own.at[r + 1, j], i
        return pltpu.make_async_remote_copy(
            src_ref=src, dst_ref=dst,
            send_sem=step_send.at[r, j, number], recv_sem=step_recv.at[r, j, number],
            device_id={"tm": device_t, "space": target}, device_id_type=MESH,
        )

    def one_source(n, carry):
        r, j = n // 2, lax.rem(n, 2)
        for d in range(SLOTS):

            @pl.when(n == 2 * d)
            def _():
                for copy in source_halos[d]:
                    copy.wait_recv()

        @pl.when(r > 0)
        def _():
            for number in range(3):
                hop(number, after, r - 1, j).wait_recv()

        @pl.when(r < SLOTS)
        def _():
            d = jnp.minimum(r, SLOTS - 1)
            take = jnp.where(r == 0, 1, 0)
            for late_by in range(1, SLOTS):
                take = jnp.where(r == late_by, here[late_by], take)
            inject = jnp.full((16, 128), take, jnp.int32) > 0
            for part in range(6):
                arrived = jnp.concatenate([recv_own[r, j, x, part] for x in range(2)], axis=0)
                for place, begun, came in (
                    (0, low_src, recv_low[r, j, part].astype(F32)),
                    (2, own_src, arrived),
                    (4, high_src, recv_high[r, j, part].astype(F32)),
                ):
                    value = jnp.where(inject, begun[d, j, part].astype(F32), came)
                    field[place, part] = value[0:8]
                    field[place + 1, part] = value[8:16]

        @pl.when(r >= SLOTS)
        def _():
            for part in range(6):
                for place, came in ((0, recv_low), (4, recv_high)):
                    value = came[r, j, part].astype(F32)
                    field[place, part] = value[0:8]
                    field[place + 1, part] = value[8:16]
                for x in range(2):
                    field[2 + x, part] = recv_own[r, j, x, part]

        on_lane = lax.rem(t - r + 2 * n_tm, n_tm)
        weight = jnp.float32(0)
        for k in range(SLOTS):
            weight = jnp.where(lane[k] == on_lane, 0.5 * coef_ref[k, j], weight)

        for q in range(4):
            half = relaxed(field, q + 1, q, weight)
            re, im = adjoint_times(lambda ri, a, b: link_t[q, ri, a, b], half)
            turned[q, 0:3] = re
            turned[q, 3:6] = im
        results = []
        for x in range(2):
            re, im = relaxed(turned, x + 1, x + 1, weight)
            sent_own[r, j, x, 0:3] = re
            sent_own[r, j, x, 3:6] = im
            results.append((re, im))
        for ri in range(2):
            both = jnp.concatenate([results[0][ri], results[1][ri]], axis=1)
            record[r, j, 3 * ri : 3 * ri + 3] = both.astype(BF16)

        @pl.when(r < rounds - 1)
        def _():
            for number in range(3):
                hop(number, after, r, j).start()

        return carry

    lax.fori_loop(0, 2 * rounds, one_source, 0)

    for k in range(SLOTS):
        round_of = late[k] + modulo(t - start[k], n_tm)
        for j in range(2):
            for ri in range(2):
                for c in range(3):
                    spot = ((k * 2 + j) * 2 + ri) * 16
                    chosen[c, spot : spot + 16] = record[round_of, j, ri * 3 + c]
    row = lax.broadcasted_iota(jnp.int32, (16, 256), 0)
    col = lax.rem(lax.broadcasted_iota(jnp.int32, (16, 256), 1), 16)
    same = jnp.where(row == 2 * lax.rem(col, 8) + col // 8, 1.0, 0.0).astype(F32)
    n_sinks = sinks.shape[1]

    def some_sinks(step, carry):
        first = pl.multiple_of(step * 16, 16)
        for ri in range(2):
            products = None
            for c in range(3):
                block = sinks[ri, pl.ds(first, 16), c].reshape(256, 128)
                product = lax.dot_general(
                    block, chosen[c], (((1,), (1,)), ((), ())), preferred_element_type=F32
                )
                products = product if products is None else products + product
            products = products.reshape(16, 16, 256) * same[None]
            summed[ri, pl.ds(first, 16), :] = jnp.sum(products, axis=1)
        return carry

    lax.fori_loop(0, n_sinks // 16, some_sinks, 0)
    entry = lax.broadcasted_iota(jnp.int32, (256, 128), 0) // 16
    column = lax.broadcasted_iota(jnp.int32, (256, 128), 1)
    field_ri, field_v = lax.rem(entry, 2), entry // 2
    from_re = jnp.where(column == field_ri * 8 + field_v, 1.0, 0.0)
    from_im = jnp.where(column == (1 - field_ri) * 8 + field_v, 1.0, 0.0)
    from_im = from_im * jnp.where(field_ri == 1, 1.0, -1.0)
    partial[...] = jnp.dot(
        summed[0], from_re.astype(F32), precision=lax.Precision.HIGHEST, preferred_element_type=F32
    ) + jnp.dot(
        summed[1], from_im.astype(F32), precision=lax.Precision.HIGHEST, preferred_element_type=F32
    )

    share = n_sinks // n_space

    def give(step):
        target = lax.rem(i + step, n_space)
        return pltpu.make_async_remote_copy(
            src_ref=partial.at[pl.ds(pl.multiple_of(target * share, share), share)],
            dst_ref=parts.at[step],
            send_sem=part_send.at[step], recv_sem=part_recv.at[step],
            device_id={"tm": t, "space": target}, device_id_type=MESH,
        )

    for step in range(1, n_space):
        give(step).start()
    total = partial[pl.ds(pl.multiple_of(i * share, share), share), :]
    for step in range(1, n_space):
        give(step).wait_recv()
        total = total + parts[step]
    out_ref[...] = total

    for step in range(1, n_space):
        give(step).wait_send()
    for copy in link_halos + source_halos[0] + source_halos[1] + source_halos[2] + source_halos[3]:
        copy.wait_send()

    def finish(n, carry):
        for number in range(3):
            hop(number, after, n // 2, lax.rem(n, 2)).wait_send()
        return carry

    lax.fori_loop(0, 2 * (rounds - 1), finish, 0)


def rows_of(x):
    lead = x.shape[:-2]
    x = x.reshape(*lead, 2, 8, 128)
    x = jnp.swapaxes(x, x.ndim - 3, x.ndim - 2)
    return x.reshape(*lead, 16, 128)


def local(gauge_links, time_links, sink_vectors, source_times, source_index, kinetic_coef):
    n_tm, n_space = lax.axis_size("tm"), lax.axis_size("space")
    n_sinks = sink_vectors.shape[2]
    rounds = n_tm + SLOTS - 1
    share = n_sinks // n_space
    smem = pl.BlockSpec(memory_space=pltpu.SMEM)
    hbm = pl.BlockSpec(memory_space=pl.ANY)
    vmem = pltpu.VMEM
    dma = pltpu.SemaphoreType.DMA
    result = pl.pallas_call(
        functools.partial(kernel, n_tm, n_space, rounds),
        out_shape=jax.ShapeDtypeStruct((share, 128), F32),
        in_specs=[smem, smem, smem, hbm, hbm, hbm],
        out_specs=pl.BlockSpec(memory_space=pltpu.VMEM),
        scratch_shapes=[
            vmem((2, 3, 3, 3, 16, 128), F32),
            vmem((2, 3, 3, 16, 128), F32),
            vmem((2, n_sinks, 3, 16, 128), BF16),
            vmem((5, 2, 3, 3, 8, 128), F32),
            vmem((4, 2, 2, 3, 3, 8, 128), F32),
            vmem((4, 2, 3, 3, 8, 128), F32),
            vmem((45, 16, 128), BF16),
            vmem((36, 16, 128), BF16),
            vmem((45, 16, 128), BF16),
            vmem((36, 16, 128), BF16),
            vmem((SLOTS, 2, 6, 16, 128), F32),
            vmem((SLOTS, 2, 6, 16, 128), BF16),
            vmem((SLOTS, 2, 6, 16, 128), BF16),
            vmem((SLOTS, 2, 6, 16, 128), BF16),
            vmem((rounds, 2, 2, 6, 8, 128), F32),
            vmem((rounds, 2, 6, 16, 128), BF16),
            vmem((rounds, 2, 6, 16, 128), BF16),
            vmem((rounds, 2, 2, 6, 8, 128), F32),
            vmem((rounds, 2, 6, 16, 128), BF16),
            vmem((6, 6, 8, 128), F32),
            vmem((4, 6, 8, 128), F32),
            vmem((3, 256, 128), BF16),
            vmem((2, n_sinks, 256), F32),
            vmem((n_sinks, 128), F32),
            vmem((n_space, share, 128), F32),
            dma((3,)),
            dma((2 * SLOTS + 2,)),
            dma((2 * SLOTS + 2,)),
            dma((rounds - 1, 2, 3)),
            dma((rounds - 1, 2, 3)),
            dma((n_space,)),
            dma((n_space,)),
        ],
        compiler_params=pltpu.CompilerParams(collective_id=0, has_side_effects=True),
    )(
        source_times, source_index, kinetic_coef,
        rows_of(gauge_links[0]), rows_of(time_links[0]), rows_of(sink_vectors[0]),
    )
    groups, per_group = kinetic_coef.shape
    table = result[:, : 2 * groups * per_group].reshape(share, 2, groups, per_group)
    return jnp.moveaxis(table, 0, 3)[:, :, :, None, :]


def solution(mesh):
    placed = (
        P("tm", None, None, None, None, "space", None),
        P("tm", None, None, None, "space", None),
        P("tm", None, None, None, "space", None),
        P(),
        P(),
        P(),
    )
    return jax.shard_map(
        local,
        mesh=mesh,
        in_specs=placed,
        out_specs=P(None, None, None, "tm", "space"),
        check_vma=False,
    )
```

```python
import functools

import jax
import jax.numpy as jnp
from jax import lax
from jax.experimental import pallas as pl
from jax.experimental.pallas import tpu as pltpu
from jax.sharding import PartitionSpec as P

MESH = pl.DeviceIdType.MESH
F32 = jnp.float32
BF16 = jnp.bfloat16
SLOTS = 4


def modulo(value, length):
    return jnp.where(value < 0, value + length, value)


def schedule(start, n_tm):
    late, lane = [], []
    for k in range(SLOTS):
        free = []
        for d in range(SLOTS - 1):
            place = modulo(start[k] - d, n_tm)
            ok = jnp.int32(1)
            for other in lane:
                ok = jnp.where(other == place, 0, ok)
            free.append(ok)
        d = jnp.int32(SLOTS - 1)
        for value in reversed(range(SLOTS - 1)):
            d = jnp.where(free[value] == 1, value, d)
        late.append(d)
        lane.append(modulo(start[k] - d, n_tm))
    return late, lane


def times(links, field):
    real, imag = None, None
    for b in range(3):
        u_re, u_im = links(0, slice(None), b), links(1, slice(None), b)
        f_re, f_im = field[0][b : b + 1], field[1][b : b + 1]
        re = u_re * f_re - u_im * f_im
        im = u_re * f_im + u_im * f_re
        real, imag = (re, im) if real is None else (real + re, imag + im)
    return real, imag


def adjoint_times(links, field):
    real, imag = None, None
    for b in range(3):
        u_re, u_im = links(0, b, slice(None)), links(1, b, slice(None))
        f_re, f_im = field[0][b : b + 1], field[1][b : b + 1]
        re = u_re * f_re + u_im * f_im
        im = u_re * f_im - u_im * f_re
        real, imag = (re, im) if real is None else (real + re, imag + im)
    return real, imag


def kernel(
    n_tm, n_space, slots,
    times_ref, index_ref, coef_ref, gauge_hbm, temporal_hbm, sinks_hbm,
    out_ref,
    gauge_in, temporal_in, sinks, link_x, link_yz, link_t,
    up_out, down_out, low_links, high_links,
    staged, own_src, low_src, high_src,
    recv_own, recv_low, recv_high, sent_own, record,
    field, turned, chosen, summed, partial, parts,
    local_sem, halo_send, halo_recv, step_send, step_recv, part_send, part_recv,
):
    rounds = n_tm + slots - 1
    t = lax.axis_index("tm")
    i = lax.axis_index("space")
    after, before = lax.rem(t + 1, n_tm), lax.rem(t + n_tm - 1, n_tm)
    above, below = lax.rem(i + 1, n_space), lax.rem(i + n_space - 1, n_space)

    fetches = [
        pltpu.make_async_copy(gauge_hbm, gauge_in, local_sem.at[0]),
        pltpu.make_async_copy(temporal_hbm, temporal_in, local_sem.at[1]),
        pltpu.make_async_copy(sinks_hbm, sinks, local_sem.at[2]),
    ]
    for fetch in fetches:
        fetch.start()

    barrier = pltpu.get_barrier_semaphore()
    for near_t in (before, after):
        for near_i in (below, i, above):
            pl.semaphore_signal(
                barrier, inc=1, device_id={"tm": near_t, "space": near_i}, device_id_type=MESH
            )
    for step in range(1, n_space):
        pl.semaphore_signal(
            barrier, inc=1,
            device_id={"tm": t, "space": lax.rem(i + step, n_space)}, device_id_type=MESH,
        )

    recv_own[0] = jnp.zeros_like(recv_own[0])
    recv_low[0] = jnp.zeros_like(recv_low[0])
    recv_high[0] = jnp.zeros_like(recv_high[0])

    start = [times_ref[k] for k in range(SLOTS)]
    late, lane = schedule(start, n_tm)
    here, which = [], []
    for d in range(SLOTS):
        count = jnp.int32(0)
        index = [jnp.int32(0), jnp.int32(0)]
        for k in range(SLOTS):
            match = jnp.where(start[k] == t, jnp.where(late[k] == d, 1, 0), 0)
            count = count + match
            index = [index[j] + match * index_ref[j, k] for j in range(2)]
        here.append(count)
        which.append(index)

    fetches[0].wait()
    fetches[1].wait()
    for x in range(2):
        for row in range(3):
            for col in range(3):
                for mu in range(4):
                    pair = []
                    for ri in range(2):
                        if mu == 3:
                            plane = temporal_in[ri, row, col, pl.ds(x, 8, stride=2), :]
                            link_t[1 + x, ri, row, col] = plane
                        else:
                            plane = gauge_in[ri, mu, row, col, pl.ds(x, 8, stride=2), :]
                            if mu == 0:
                                link_x[2 + x, ri, row, col] = plane
                            else:
                                link_yz[1 + x, mu - 1, ri, row, col] = plane
                        pair.append(plane)
                    if row < 2:
                        packed = jnp.concatenate(pair, axis=0).astype(BF16)
                        if x == 1:
                            up_out[mu, row * 3 + col] = packed
                        else:
                            down_out[mu, row * 3 + col] = packed
                            if mu == 0:
                                up_out[4, row * 3 + col] = packed

    pl.semaphore_wait(barrier, 6 + n_space - 1)

    def halo(number, src, dst, device):
        return pltpu.make_async_remote_copy(
            src_ref=src, dst_ref=dst, send_sem=halo_send.at[number], recv_sem=halo_recv.at[number],
            device_id={"tm": t, "space": device}, device_id_type=MESH,
        )

    link_halos = (
        halo(2 * SLOTS, up_out, low_links, above),
        halo(2 * SLOTS + 1, down_out, high_links, below),
    )
    for copy in link_halos:
        copy.start()

    fetches[2].wait()
    source_halos = []
    for d in range(slots):
        keep = here[d].astype(F32)
        for j in range(2):
            for ri in range(2):
                for c in range(3):
                    staged[d, j, ri * 3 + c] = sinks[ri, which[d][j], c].astype(F32) * keep
            for part in range(6):
                planes = [staged[d, j, part, pl.ds(x, 8, stride=2), :] for x in range(2)]
                own_src[d, j, part] = jnp.concatenate(planes, axis=0).astype(BF16)
        source_halos.append(
            (
                halo(2 * d, own_src.at[d], low_src.at[d], above),
                halo(2 * d + 1, own_src.at[d], high_src.at[d], below),
            )
        )
        for copy in source_halos[d]:
            copy.start()

    def unpack(packed, store):
        rows = [[packed[row * 3 + col].astype(F32) for col in range(3)] for row in range(2)]
        re = [[entry[0:8] for entry in row] for row in rows]
        im = [[entry[8:16] for entry in row] for row in rows]
        last_re, last_im = [], []
        for col in range(3):
            a, b = (col + 1) % 3, (col + 2) % 3
            last_re.append(
                (re[0][a] * re[1][b] - im[0][a] * im[1][b]) - (re[0][b] * re[1][a] - im[0][b] * im[1][a])
            )
            last_im.append(
                (re[0][b] * im[1][a] + im[0][b] * re[1][a]) - (re[0][a] * im[1][b] + im[0][a] * re[1][b])
            )
        re, im = re + [last_re], im + [last_im]
        for row in range(3):
            for col in range(3):
                store[0, row, col] = re[row][col]
                store[1, row, col] = im[row][col]

    link_halos[0].wait_recv()
    link_halos[1].wait_recv()
    for arrived, x_plane, plane in ((low_links, 1, 0), (high_links, 4, 3)):
        unpack(arrived.at[0], link_x.at[x_plane])
        unpack(arrived.at[1], link_yz.at[plane, 0])
        unpack(arrived.at[2], link_yz.at[plane, 1])
        unpack(arrived.at[3], link_t.at[plane])
    unpack(low_links.at[4], link_x.at[0])

    lanes = lax.broadcasted_iota(jnp.int32, (3, 8, 128), 2)
    z = lax.rem(lanes, 32)
    first_z, last_z = z == 0, z == 31
    low_lanes, high_lanes = lanes < 32, lanes >= 96

    def up(values, direction):
        if direction == 0:
            moved = pltpu.roll(values, 96, 2)
            return jnp.where(high_lanes, pltpu.roll(moved, 7, 1), moved)
        return jnp.where(last_z, pltpu.roll(values, 31, 2), pltpu.roll(values, 127, 2))

    def down(values, direction):
        if direction == 0:
            moved = pltpu.roll(values, 32, 2)
            return jnp.where(low_lanes, pltpu.roll(moved, 1, 1), moved)
        return jnp.where(first_z, pltpu.roll(values, 97, 2), pltpu.roll(values, 1, 2))

    def relaxed(source, q, links_q, weight):
        at = lambda p: (source[p, 0:3], source[p, 3:6])
        centre = at(q)
        re, im = times(lambda ri, a, b: link_x[links_q + 1, ri, a, b], at(q + 1))
        more = adjoint_times(lambda ri, a, b: link_x[links_q, ri, a, b], at(q - 1))
        re, im = re + more[0], im + more[1]
        for direction in range(2):
            links = lambda ri, a, b: link_yz[links_q, direction, ri, a, b]
            more = times(links, tuple(up(part, direction) for part in centre))
            re, im = re + more[0], im + more[1]
            more = tuple(down(part, direction) for part in adjoint_times(links, centre))
            re, im = re + more[0], im + more[1]
        rest = 1.0 - 6.0 * weight
        return rest * centre[0] + weight * re, rest * centre[1] + weight * im

    def hop(number, device_t, r, j):
        if number == 0:
            src, dst, target = record.at[r, j], recv_low.at[r + 1, j], above
        elif number == 1:
            src, dst, target = record.at[r, j], recv_high.at[r + 1, j], below
        else:
            src, dst, target = sent_own.at[r, j], recv_own.at[r + 1, j], i
        return pltpu.make_async_remote_copy(
            src_ref=src, dst_ref=dst,
            send_sem=step_send.at[r, j, number], recv_sem=step_recv.at[r, j, number],
            device_id={"tm": device_t, "space": target}, device_id_type=MESH,
        )

    def one_source(n, carry):
        r, j = n // 2, lax.rem(n, 2)
        for d in range(slots):

            @pl.when(n == 2 * d)
            def _():
                for copy in source_halos[d]:
                    copy.wait_recv()

        @pl.when(r > 0)
        def _():
            for number in range(3):
                hop(number, after, r - 1, j).wait_recv()

        @pl.when(r < slots)
        def _():
            d = jnp.minimum(r, slots - 1)
            take = jnp.where(r == 0, 1, 0)
            for late_by in range(1, slots):
                take = jnp.where(r == late_by, here[late_by], take)
            inject = jnp.full((16, 128), take, jnp.int32) > 0
            for part in range(6):
                arrived = jnp.concatenate([recv_own[r, j, x, part] for x in range(2)], axis=0)
                for place, begun, came in (
                    (0, low_src, recv_low[r, j, part].astype(F32)),
                    (2, own_src, arrived),
                    (4, high_src, recv_high[r, j, part].astype(F32)),
                ):
                    value = jnp.where(inject, begun[d, j, part].astype(F32), came)
                    field[place, part] = value[0:8]
                    field[place + 1, part] = value[8:16]

        @pl.when(r >= slots)
        def _():
            for part in range(6):
                for place, came in ((0, recv_low), (4, recv_high)):
                    value = came[r, j, part].astype(F32)
                    field[place, part] = value[0:8]
                    field[place + 1, part] = value[8:16]
                for x in range(2):
                    field[2 + x, part] = recv_own[r, j, x, part]

        on_lane = lax.rem(t - r + 2 * n_tm, n_tm)
        weight = jnp.float32(0)
        for k in range(SLOTS):
            weight = jnp.where(lane[k] == on_lane, 0.5 * coef_ref[j, k], weight)

        for q in range(4):
            half = relaxed(field, q + 1, q, weight)
            re, im = adjoint_times(lambda ri, a, b: link_t[q, ri, a, b], half)
            turned[q, 0:3] = re
            turned[q, 3:6] = im
        results = []
        for x in range(2):
            re, im = relaxed(turned, x + 1, x + 1, weight)
            sent_own[r, j, x, 0:3] = re
            sent_own[r, j, x, 3:6] = im
            results.append((re, im))
        for ri in range(2):
            both = jnp.concatenate([results[0][ri], results[1][ri]], axis=1)
            record[r, j, 3 * ri : 3 * ri + 3] = both.astype(BF16)

        @pl.when(r < rounds - 1)
        def _():
            for number in range(3):
                hop(number, after, r, j).start()

        return carry

    lax.fori_loop(0, 2 * rounds, one_source, 0)

    for k in range(SLOTS):
        round_of = jnp.minimum(late[k] + modulo(t - start[k], n_tm), rounds - 1)
        for j in range(2):
            for c in range(3):
                spot = (k * 2 + j) * 16
                re, im = record[round_of, j, c], record[round_of, j, 3 + c]
                chosen[c, spot : spot + 16] = jnp.concatenate([re, im], axis=1)
                chosen[c, 128 + spot : 128 + spot + 16] = jnp.concatenate([im, -re], axis=1)
    row = lax.broadcasted_iota(jnp.int32, (16, 256), 0)
    col = lax.rem(lax.broadcasted_iota(jnp.int32, (16, 256), 1), 16)
    same = jnp.where(row == 2 * lax.rem(col, 8) + col // 8, 1.0, 0.0).astype(F32)
    n_sinks = sinks.shape[1]

    def some_sinks(step, carry):
        first = pl.multiple_of(step * 16, 16)
        products = None
        for c in range(3):
            block = jnp.concatenate([sinks[ri, pl.ds(first, 16), c].reshape(256, 128) for ri in range(2)], axis=1)
            product = lax.dot_general(
                block, chosen[c], (((1,), (1,)), ((), ())), preferred_element_type=F32
            )
            products = product if products is None else products + product
        products = products.reshape(16, 16, 256) * same[None]
        summed[pl.ds(first, 16), :] = jnp.sum(products, axis=1)
        return carry

    lax.fori_loop(0, n_sinks // 16, some_sinks, 0)
    entry = lax.broadcasted_iota(jnp.int32, (256, 128), 0) // 16
    column = lax.broadcasted_iota(jnp.int32, (256, 128), 1)
    fold = jnp.where(entry == column, 1.0, 0.0).astype(F32)
    partial[...] = jnp.dot(
        summed[...], fold, precision=lax.Precision.HIGHEST, preferred_element_type=F32
    )

    share = n_sinks // n_space

    def give(step):
        target = lax.rem(i + step, n_space)
        return pltpu.make_async_remote_copy(
            src_ref=partial.at[pl.ds(pl.multiple_of(target * share, share), share)],
            dst_ref=parts.at[step],
            send_sem=part_send.at[step], recv_sem=part_recv.at[step],
            device_id={"tm": t, "space": target}, device_id_type=MESH,
        )

    for step in range(1, n_space):
        give(step).start()
    total = partial[pl.ds(pl.multiple_of(i * share, share), share), :]
    for step in range(1, n_space):
        give(step).wait_recv()
        total = total + parts[step]
    out_ref[...] = total

    for step in range(1, n_space):
        give(step).wait_send()
    for copy in sum(source_halos, link_halos):
        copy.wait_send()

    def finish(n, carry):
        for number in range(3):
            hop(number, after, n // 2, lax.rem(n, 2)).wait_send()
        return carry

    lax.fori_loop(0, 2 * (rounds - 1), finish, 0)


def latest_start(n_tm, times_ref, out_ref):
    late, _ = schedule([times_ref[k] for k in range(SLOTS)], n_tm)
    latest = late[0]
    for d in late[1:]:
        latest = jnp.maximum(latest, d)
    out_ref[0] = latest


def rows_of(x):
    lead = x.shape[:-2]
    x = x.reshape(*lead, 2, 8, 128)
    x = jnp.swapaxes(x, x.ndim - 3, x.ndim - 2)
    return x.reshape(*lead, 16, 128)


def local(gauge_links, time_links, sink_vectors, source_times, source_index, kinetic_coef):
    n_tm, n_space = lax.axis_size("tm"), lax.axis_size("space")
    n_sinks = sink_vectors.shape[2]
    share = n_sinks // n_space
    smem = pl.BlockSpec(memory_space=pltpu.SMEM)
    hbm = pl.BlockSpec(memory_space=pl.ANY)
    vmem = pltpu.VMEM
    dma = pltpu.SemaphoreType.DMA

    def with_slots(slots):
        rounds = n_tm + slots - 1
        return pl.pallas_call(
            functools.partial(kernel, n_tm, n_space, slots),
            out_shape=jax.ShapeDtypeStruct((share, 128), F32),
            in_specs=[smem, smem, smem, hbm, hbm, hbm],
            out_specs=pl.BlockSpec(memory_space=pltpu.VMEM),
            scratch_shapes=[
                vmem((2, 3, 3, 3, 16, 128), F32),
                vmem((2, 3, 3, 16, 128), F32),
                vmem((2, n_sinks, 3, 16, 128), BF16),
                vmem((5, 2, 3, 3, 8, 128), F32),
                vmem((4, 2, 2, 3, 3, 8, 128), F32),
                vmem((4, 2, 3, 3, 8, 128), F32),
                vmem((5, 6, 16, 128), BF16),
                vmem((4, 6, 16, 128), BF16),
                vmem((5, 6, 16, 128), BF16),
                vmem((4, 6, 16, 128), BF16),
                vmem((slots, 2, 6, 16, 128), F32),
                vmem((slots, 2, 6, 16, 128), BF16),
                vmem((slots, 2, 6, 16, 128), BF16),
                vmem((slots, 2, 6, 16, 128), BF16),
                vmem((rounds, 2, 2, 6, 8, 128), F32),
                vmem((rounds, 2, 6, 16, 128), BF16),
                vmem((rounds, 2, 6, 16, 128), BF16),
                vmem((rounds, 2, 2, 6, 8, 128), F32),
                vmem((rounds, 2, 6, 16, 128), BF16),
                vmem((6, 6, 8, 128), F32),
                vmem((4, 6, 8, 128), F32),
                vmem((3, 256, 256), BF16),
                vmem((n_sinks, 256), F32),
                vmem((n_sinks, 128), F32),
                vmem((n_space, share, 128), F32),
                dma((3,)),
                dma((2 * SLOTS + 2,)),
                dma((2 * SLOTS + 2,)),
                dma((rounds - 1, 2, 3)),
                dma((rounds - 1, 2, 3)),
                dma((n_space,)),
                dma((n_space,)),
            ],
            compiler_params=pltpu.CompilerParams(collective_id=slots - 1, has_side_effects=True),
        )

    latest = pl.pallas_call(
        functools.partial(latest_start, n_tm),
        out_shape=jax.ShapeDtypeStruct((1,), jnp.int32),
        in_specs=[smem],
        out_specs=smem,
    )(source_times)[0]
    result = lax.switch(
        latest,
        [with_slots(slots) for slots in range(1, SLOTS + 1)],
        source_times, source_index.T, kinetic_coef.T,
        rows_of(gauge_links[0]), rows_of(time_links[0]), rows_of(sink_vectors[0]),
    )
    groups, per_group = kinetic_coef.shape
    table = result[:, : 2 * groups * per_group].reshape(share, 2, groups, per_group)
    return jnp.moveaxis(table, 0, 3)[:, :, :, None, :]


def solution(mesh):
    placed = (
        P("tm", None, None, None, None, "space", None),
        P("tm", None, None, None, "space", None),
        P("tm", None, None, None, "space", None),
        P(),
        P(),
        P(),
    )
    return jax.shard_map(
        local,
        mesh=mesh,
        in_specs=placed,
        out_specs=P(None, None, None, "tm", "space"),
        check_vma=False,
    )
```

```python
import functools

import jax
import jax.numpy as jnp
from jax import lax
from jax.experimental import pallas as pl
from jax.experimental.pallas import tpu as pltpu
from jax.sharding import PartitionSpec as P

MESH = pl.DeviceIdType.MESH
F32 = jnp.float32
BF16 = jnp.bfloat16
SLOTS = 4


def modulo(value, length):
    return jnp.where(value < 0, value + length, value)


def schedule(start, n_tm):
    late, lane = [], []
    for k in range(SLOTS):
        free = []
        for d in range(SLOTS - 1):
            place = modulo(start[k] - d, n_tm)
            ok = jnp.int32(1)
            for other in lane:
                ok = jnp.where(other == place, 0, ok)
            free.append(ok)
        d = jnp.int32(SLOTS - 1)
        for value in reversed(range(SLOTS - 1)):
            d = jnp.where(free[value] == 1, value, d)
        late.append(d)
        lane.append(modulo(start[k] - d, n_tm))
    return late, lane


def times(links, field):
    real, imag = None, None
    for b in range(3):
        u_re, u_im = links(0, slice(None), b), links(1, slice(None), b)
        f_re, f_im = field[0][b : b + 1], field[1][b : b + 1]
        re = u_re * f_re - u_im * f_im
        im = u_re * f_im + u_im * f_re
        real, imag = (re, im) if real is None else (real + re, imag + im)
    return real, imag


def adjoint_times(links, field):
    real, imag = None, None
    for b in range(3):
        u_re, u_im = links(0, b, slice(None)), links(1, b, slice(None))
        f_re, f_im = field[0][b : b + 1], field[1][b : b + 1]
        re = u_re * f_re + u_im * f_im
        im = u_re * f_im - u_im * f_re
        real, imag = (re, im) if real is None else (real + re, imag + im)
    return real, imag


def kernel(
    n_tm, n_space, slots,
    times_ref, index_ref, coef_ref, gauge_hbm, temporal_hbm, sinks_hbm,
    out_ref,
    gauge_in, temporal_in, sinks, link_x, link_yz, link_t,
    up_out, down_out, low_links, high_links,
    staged, own_src, low_src, high_src,
    recv_own, recv_low, recv_high, sent_own, record,
    field, early, turned, chosen, summed, partial, parts,
    local_sem, halo_send, halo_recv, step_send, step_recv, part_send, part_recv,
):
    rounds = n_tm + slots - 1
    t = lax.axis_index("tm")
    i = lax.axis_index("space")
    after, before = lax.rem(t + 1, n_tm), lax.rem(t + n_tm - 1, n_tm)
    above, below = lax.rem(i + 1, n_space), lax.rem(i + n_space - 1, n_space)

    fetches = [
        pltpu.make_async_copy(gauge_hbm, gauge_in, local_sem.at[0]),
        pltpu.make_async_copy(temporal_hbm, temporal_in, local_sem.at[1]),
        pltpu.make_async_copy(sinks_hbm, sinks, local_sem.at[2]),
    ]
    for fetch in fetches:
        fetch.start()

    barrier = pltpu.get_barrier_semaphore()
    for near_t in (before, after):
        for near_i in (below, i, above):
            pl.semaphore_signal(
                barrier, inc=1, device_id={"tm": near_t, "space": near_i}, device_id_type=MESH
            )
    for step in range(1, n_space):
        pl.semaphore_signal(
            barrier, inc=1,
            device_id={"tm": t, "space": lax.rem(i + step, n_space)}, device_id_type=MESH,
        )

    recv_own[0] = jnp.zeros_like(recv_own[0])
    recv_low[0] = jnp.zeros_like(recv_low[0])
    recv_high[0] = jnp.zeros_like(recv_high[0])

    start = [times_ref[k] for k in range(SLOTS)]
    late, lane = schedule(start, n_tm)
    here, which = [], []
    for d in range(SLOTS):
        count = jnp.int32(0)
        index = [jnp.int32(0), jnp.int32(0)]
        for k in range(SLOTS):
            match = jnp.where(start[k] == t, jnp.where(late[k] == d, 1, 0), 0)
            count = count + match
            index = [index[j] + match * index_ref[j, k] for j in range(2)]
        here.append(count)
        which.append(index)

    fetches[0].wait()
    fetches[1].wait()
    for x in range(2):
        for row in range(3):
            for col in range(3):
                for mu in range(4):
                    pair = []
                    for ri in range(2):
                        if mu == 3:
                            plane = temporal_in[ri, row, col, pl.ds(x, 8, stride=2), :]
                            link_t[1 + x, ri, row, col] = plane
                        else:
                            plane = gauge_in[ri, mu, row, col, pl.ds(x, 8, stride=2), :]
                            if mu == 0:
                                link_x[2 + x, ri, row, col] = plane
                            else:
                                link_yz[1 + x, mu - 1, ri, row, col] = plane
                        pair.append(plane)
                    if row < 2:
                        packed = jnp.concatenate(pair, axis=0).astype(BF16)
                        if x == 1:
                            up_out[mu, row * 3 + col] = packed
                        else:
                            down_out[mu, row * 3 + col] = packed
                            if mu == 0:
                                up_out[4, row * 3 + col] = packed

    pl.semaphore_wait(barrier, 6 + n_space - 1)

    def halo(number, src, dst, device):
        return pltpu.make_async_remote_copy(
            src_ref=src, dst_ref=dst, send_sem=halo_send.at[number], recv_sem=halo_recv.at[number],
            device_id={"tm": t, "space": device}, device_id_type=MESH,
        )

    link_halos = (
        halo(2 * SLOTS, up_out, low_links, above),
        halo(2 * SLOTS + 1, down_out, high_links, below),
    )
    for copy in link_halos:
        copy.start()

    fetches[2].wait()
    source_halos = []
    for d in range(slots):
        keep = here[d].astype(F32)
        for j in range(2):
            for ri in range(2):
                for c in range(3):
                    staged[d, j, ri * 3 + c] = sinks[ri, which[d][j], c].astype(F32) * keep
            for part in range(6):
                planes = [staged[d, j, part, pl.ds(x, 8, stride=2), :] for x in range(2)]
                own_src[d, j, part] = jnp.concatenate(planes, axis=0).astype(BF16)
        source_halos.append(
            (
                halo(2 * d, own_src.at[d], low_src.at[d], above),
                halo(2 * d + 1, own_src.at[d], high_src.at[d], below),
            )
        )
        for copy in source_halos[d]:
            copy.start()

    def unpack(packed, store):
        rows = [[packed[row * 3 + col].astype(F32) for col in range(3)] for row in range(2)]
        re = [[entry[0:8] for entry in row] for row in rows]
        im = [[entry[8:16] for entry in row] for row in rows]
        last_re, last_im = [], []
        for col in range(3):
            a, b = (col + 1) % 3, (col + 2) % 3
            last_re.append(
                (re[0][a] * re[1][b] - im[0][a] * im[1][b]) - (re[0][b] * re[1][a] - im[0][b] * im[1][a])
            )
            last_im.append(
                (re[0][b] * im[1][a] + im[0][b] * re[1][a]) - (re[0][a] * im[1][b] + im[0][a] * re[1][b])
            )
        re, im = re + [last_re], im + [last_im]
        for row in range(3):
            for col in range(3):
                store[0, row, col] = re[row][col]
                store[1, row, col] = im[row][col]

    link_halos[0].wait_recv()
    link_halos[1].wait_recv()
    for arrived, x_plane, plane in ((low_links, 1, 0), (high_links, 4, 3)):
        unpack(arrived.at[0], link_x.at[x_plane])
        unpack(arrived.at[1], link_yz.at[plane, 0])
        unpack(arrived.at[2], link_yz.at[plane, 1])
        unpack(arrived.at[3], link_t.at[plane])
    unpack(low_links.at[4], link_x.at[0])

    lanes = lax.broadcasted_iota(jnp.int32, (3, 8, 128), 2)
    z = lax.rem(lanes, 32)
    first_z, last_z = z == 0, z == 31
    low_lanes, high_lanes = lanes < 32, lanes >= 96

    def up(values, direction):
        if direction == 0:
            moved = pltpu.roll(values, 96, 2)
            return jnp.where(high_lanes, pltpu.roll(moved, 7, 1), moved)
        return jnp.where(last_z, pltpu.roll(values, 31, 2), pltpu.roll(values, 127, 2))

    def down(values, direction):
        if direction == 0:
            moved = pltpu.roll(values, 32, 2)
            return jnp.where(low_lanes, pltpu.roll(moved, 1, 1), moved)
        return jnp.where(first_z, pltpu.roll(values, 97, 2), pltpu.roll(values, 1, 2))

    def neighbours(source, q, links_q, total=None, x_up=True, x_down=True, flat=True):
        at = lambda p: (source[p, 0:3], source[p, 3:6])

        def plus(more):
            return more if total is None else (total[0] + more[0], total[1] + more[1])

        if flat:
            centre = at(q)
            for direction in range(2):
                links = lambda ri, a, b: link_yz[links_q, direction, ri, a, b]
                total = plus(times(links, tuple(up(part, direction) for part in centre)))
                total = plus(tuple(down(part, direction) for part in adjoint_times(links, centre)))
        if x_up:
            total = plus(times(lambda ri, a, b: link_x[links_q + 1, ri, a, b], at(q + 1)))
        if x_down:
            total = plus(adjoint_times(lambda ri, a, b: link_x[links_q, ri, a, b], at(q - 1)))
        return total

    def relaxed(source, q, total, weight):
        rest = 1.0 - 6.0 * weight
        return rest * source[q, 0:3] + weight * total[0], rest * source[q, 3:6] + weight * total[1]

    def hop(number, device_t, r, j):
        if number == 0:
            src, dst, target = record.at[r, j], recv_low.at[r + 1, j], above
        elif number == 1:
            src, dst, target = record.at[r, j], recv_high.at[r + 1, j], below
        else:
            src, dst, target = sent_own.at[r, j], recv_own.at[r + 1, j], i
        return pltpu.make_async_remote_copy(
            src_ref=src, dst_ref=dst,
            send_sem=step_send.at[r, j, number], recv_sem=step_recv.at[r, j, number],
            device_id={"tm": device_t, "space": target}, device_id_type=MESH,
        )

    def one_source(n, carry):
        r, j = n // 2, lax.rem(n, 2)
        for d in range(slots):

            @pl.when(n == 2 * d)
            def _():
                for copy in source_halos[d]:
                    copy.wait_recv()

        d = jnp.minimum(r, slots - 1)
        take = jnp.where(r == 0, 1, 0)
        for late_by in range(1, slots):
            take = jnp.where(r == late_by, here[late_by], take)

        @pl.when(r > 0)
        def _():
            hop(2, after, r - 1, j).wait_recv()

        @pl.when(r < slots)
        def _():
            inject = jnp.full((16, 128), take, jnp.int32) > 0
            for part in range(6):
                arrived = jnp.concatenate([recv_own[r, j, x, part] for x in range(2)], axis=0)
                value = jnp.where(inject, own_src[d, j, part].astype(F32), arrived)
                field[2, part] = value[0:8]
                field[3, part] = value[8:16]

        @pl.when(r >= slots)
        def _():
            for part in range(6):
                for x in range(2):
                    field[2 + x, part] = recv_own[r, j, x, part]

        for q in (1, 2):
            re, im = neighbours(field, q + 1, q, x_up=q == 1, x_down=q == 2)
            early[q - 1, 0:3] = re
            early[q - 1, 3:6] = im

        @pl.when(r > 0)
        def _():
            for number in range(2):
                hop(number, after, r - 1, j).wait_recv()

        @pl.when(r < slots)
        def _():
            inject = jnp.full((16, 128), take, jnp.int32) > 0
            for part in range(6):
                for place, begun, came in ((0, low_src, recv_low), (4, high_src, recv_high)):
                    value = jnp.where(inject, begun[d, j, part], came[r, j, part]).astype(F32)
                    field[place, part] = value[0:8]
                    field[place + 1, part] = value[8:16]

        @pl.when(r >= slots)
        def _():
            for part in range(6):
                for place, came in ((0, recv_low), (4, recv_high)):
                    value = came[r, j, part].astype(F32)
                    field[place, part] = value[0:8]
                    field[place + 1, part] = value[8:16]

        on_lane = lax.rem(t - r + 2 * n_tm, n_tm)
        weight = jnp.float32(0)
        for k in range(SLOTS):
            weight = jnp.where(lane[k] == on_lane, 0.5 * coef_ref[j, k], weight)

        for q in range(4):
            if q == 0 or q == 3:
                total = neighbours(field, q + 1, q)
            else:
                total = neighbours(
                    field, q + 1, q, (early[q - 1, 0:3], early[q - 1, 3:6]),
                    x_up=q == 2, x_down=q == 1, flat=False,
                )
            half = relaxed(field, q + 1, total, weight)
            re, im = adjoint_times(lambda ri, a, b: link_t[q, ri, a, b], half)
            turned[q, 0:3] = re
            turned[q, 3:6] = im
        results = []
        for x in range(2):
            re, im = relaxed(turned, x + 1, neighbours(turned, x + 1, x + 1), weight)
            sent_own[r, j, x, 0:3] = re
            sent_own[r, j, x, 3:6] = im
            results.append((re, im))
        for ri in range(2):
            both = jnp.concatenate([results[0][ri], results[1][ri]], axis=1)
            record[r, j, 3 * ri : 3 * ri + 3] = both.astype(BF16)

        @pl.when(r < rounds - 1)
        def _():
            for number in range(3):
                hop(number, after, r, j).start()

        return carry

    lax.fori_loop(0, 2 * rounds, one_source, 0)

    for k in range(SLOTS):
        round_of = jnp.minimum(late[k] + modulo(t - start[k], n_tm), rounds - 1)
        for j in range(2):
            for c in range(3):
                spot = (k * 2 + j) * 16
                re, im = record[round_of, j, c], record[round_of, j, 3 + c]
                chosen[c, spot : spot + 16] = jnp.concatenate([re, im], axis=1)
                chosen[c, 128 + spot : 128 + spot + 16] = jnp.concatenate([im, -re], axis=1)
    row = lax.broadcasted_iota(jnp.int32, (16, 256), 0)
    col = lax.rem(lax.broadcasted_iota(jnp.int32, (16, 256), 1), 16)
    same = jnp.where(row == 2 * lax.rem(col, 8) + col // 8, 1.0, 0.0).astype(F32)
    n_sinks = sinks.shape[1]

    def some_sinks(step, carry):
        first = pl.multiple_of(step * 64, 64)
        products = None
        for c in range(3):
            block = jnp.concatenate([sinks[ri, pl.ds(first, 64), c].reshape(1024, 128) for ri in range(2)], axis=1)
            product = lax.dot_general(
                block, chosen[c], (((1,), (1,)), ((), ())), preferred_element_type=F32
            )
            products = product if products is None else products + product
        products = products.reshape(64, 16, 256) * same[None]
        summed[pl.ds(first, 64), :] = jnp.sum(products, axis=1)
        return carry

    lax.fori_loop(0, n_sinks // 64, some_sinks, 0, unroll=False)
    entry = lax.broadcasted_iota(jnp.int32, (256, 128), 0) // 16
    column = lax.broadcasted_iota(jnp.int32, (256, 128), 1)
    fold = jnp.where(entry == column, 1.0, 0.0).astype(F32)
    partial[...] = jnp.dot(
        summed[...], fold, precision=lax.Precision.HIGHEST, preferred_element_type=F32
    )

    share = n_sinks // n_space

    def give(step):
        target = lax.rem(i + step, n_space)
        return pltpu.make_async_remote_copy(
            src_ref=partial.at[pl.ds(pl.multiple_of(target * share, share), share)],
            dst_ref=parts.at[step],
            send_sem=part_send.at[step], recv_sem=part_recv.at[step],
            device_id={"tm": t, "space": target}, device_id_type=MESH,
        )

    for step in range(1, n_space):
        give(step).start()
    total = partial[pl.ds(pl.multiple_of(i * share, share), share), :]
    for step in range(1, n_space):
        give(step).wait_recv()
        total = total + parts[step]
    out_ref[...] = total

    for step in range(1, n_space):
        give(step).wait_send()
    for copy in sum(source_halos, link_halos):
        copy.wait_send()

    def finish(n, carry):
        for number in range(3):
            hop(number, after, n // 2, lax.rem(n, 2)).wait_send()
        return carry

    lax.fori_loop(0, 2 * (rounds - 1), finish, 0)


def latest_start(n_tm, times_ref, out_ref):
    late, _ = schedule([times_ref[k] for k in range(SLOTS)], n_tm)
    latest = late[0]
    for d in late[1:]:
        latest = jnp.maximum(latest, d)
    out_ref[0] = latest


def rows_of(x):
    lead = x.shape[:-2]
    x = x.reshape(*lead, 2, 8, 128)
    x = jnp.swapaxes(x, x.ndim - 3, x.ndim - 2)
    return x.reshape(*lead, 16, 128)


def local(gauge_links, time_links, sink_vectors, source_times, source_index, kinetic_coef):
    n_tm, n_space = lax.axis_size("tm"), lax.axis_size("space")
    n_sinks = sink_vectors.shape[2]
    share = n_sinks // n_space
    smem = pl.BlockSpec(memory_space=pltpu.SMEM)
    hbm = pl.BlockSpec(memory_space=pl.ANY)
    vmem = pltpu.VMEM
    dma = pltpu.SemaphoreType.DMA

    def with_slots(slots):
        rounds = n_tm + slots - 1
        return pl.pallas_call(
            functools.partial(kernel, n_tm, n_space, slots),
            out_shape=jax.ShapeDtypeStruct((share, 128), F32),
            in_specs=[smem, smem, smem, hbm, hbm, hbm],
            out_specs=pl.BlockSpec(memory_space=pltpu.VMEM),
            scratch_shapes=[
                vmem((2, 3, 3, 3, 16, 128), F32),
                vmem((2, 3, 3, 16, 128), F32),
                vmem((2, n_sinks, 3, 16, 128), BF16),
                vmem((5, 2, 3, 3, 8, 128), F32),
                vmem((4, 2, 2, 3, 3, 8, 128), F32),
                vmem((4, 2, 3, 3, 8, 128), F32),
                vmem((5, 6, 16, 128), BF16),
                vmem((4, 6, 16, 128), BF16),
                vmem((5, 6, 16, 128), BF16),
                vmem((4, 6, 16, 128), BF16),
                vmem((slots, 2, 6, 16, 128), F32),
                vmem((slots, 2, 6, 16, 128), BF16),
                vmem((slots, 2, 6, 16, 128), BF16),
                vmem((slots, 2, 6, 16, 128), BF16),
                vmem((rounds, 2, 2, 6, 8, 128), F32),
                vmem((rounds, 2, 6, 16, 128), BF16),
                vmem((rounds, 2, 6, 16, 128), BF16),
                vmem((rounds, 2, 2, 6, 8, 128), F32),
                vmem((rounds, 2, 6, 16, 128), BF16),
                vmem((6, 6, 8, 128), F32),
                vmem((2, 6, 8, 128), F32),
                vmem((4, 6, 8, 128), F32),
                vmem((3, 256, 256), BF16),
                vmem((n_sinks, 256), F32),
                vmem((n_sinks, 128), F32),
                vmem((n_space, share, 128), F32),
                dma((3,)),
                dma((2 * SLOTS + 2,)),
                dma((2 * SLOTS + 2,)),
                dma((rounds - 1, 2, 3)),
                dma((rounds - 1, 2, 3)),
                dma((n_space,)),
                dma((n_space,)),
            ],
            compiler_params=pltpu.CompilerParams(collective_id=slots - 1, has_side_effects=True),
        )

    latest = pl.pallas_call(
        functools.partial(latest_start, n_tm),
        out_shape=jax.ShapeDtypeStruct((1,), jnp.int32),
        in_specs=[smem],
        out_specs=smem,
    )(source_times)[0]
    result = lax.switch(
        latest,
        [with_slots(slots) for slots in range(1, SLOTS + 1)],
        source_times, source_index.T, kinetic_coef.T,
        rows_of(gauge_links[0]), rows_of(time_links[0]), rows_of(sink_vectors[0]),
    )
    groups, per_group = kinetic_coef.shape
    table = result[:, : 2 * groups * per_group].reshape(share, 2, groups, per_group)
    return jnp.moveaxis(table, 0, 3)[:, :, :, None, :]


def solution(mesh):
    placed = (
        P("tm", None, None, None, None, "space", None),
        P("tm", None, None, None, "space", None),
        P("tm", None, None, None, "space", None),
        P(),
        P(),
        P(),
    )
    return jax.shard_map(
        local,
        mesh=mesh,
        in_specs=placed,
        out_specs=P(None, None, None, "tm", "space"),
        check_vma=False,
    )
```

```python
import functools

import jax
import jax.numpy as jnp
from jax import lax
from jax.experimental import pallas as pl
from jax.experimental.pallas import tpu as pltpu
from jax.sharding import PartitionSpec as P

MESH = pl.DeviceIdType.MESH
F32 = jnp.float32
BF16 = jnp.bfloat16
SLOTS = 4


def modulo(value, length):
    return jnp.where(value < 0, value + length, value)


def schedule(start, n_tm):
    late, lane = [], []
    for k in range(SLOTS):
        free = []
        for d in range(SLOTS - 1):
            place = modulo(start[k] - d, n_tm)
            ok = jnp.int32(1)
            for other in lane:
                ok = jnp.where(other == place, 0, ok)
            free.append(ok)
        d = jnp.int32(SLOTS - 1)
        for value in reversed(range(SLOTS - 1)):
            d = jnp.where(free[value] == 1, value, d)
        late.append(d)
        lane.append(modulo(start[k] - d, n_tm))
    return late, lane


def times(links, field):
    real, imag = None, None
    for b in range(3):
        u_re, u_im = links(0, slice(None), b), links(1, slice(None), b)
        f_re, f_im = field[0][b : b + 1], field[1][b : b + 1]
        re = u_re * f_re - u_im * f_im
        im = u_re * f_im + u_im * f_re
        real, imag = (re, im) if real is None else (real + re, imag + im)
    return real, imag


def adjoint_times(links, field):
    real, imag = None, None
    for b in range(3):
        u_re, u_im = links(0, b, slice(None)), links(1, b, slice(None))
        f_re, f_im = field[0][b : b + 1], field[1][b : b + 1]
        re = u_re * f_re + u_im * f_im
        im = u_re * f_im - u_im * f_re
        real, imag = (re, im) if real is None else (real + re, imag + im)
    return real, imag


def kernel(
    n_tm, n_space, slots,
    times_ref, index_ref, coef_ref, gauge_hbm, temporal_hbm, sinks_hbm,
    out_ref,
    gauge_in, temporal_in, sinks, link_x, link_yz, link_t,
    up_out, down_out, low_links, high_links,
    staged, own_src, low_src, high_src,
    recv_own, recv_low, recv_high, sent_own, record,
    field, early, turned, chosen, summed, partial, parts,
    local_sem, halo_send, halo_recv, step_send, step_recv, part_send, part_recv,
):
    rounds = n_tm + slots - 1
    t = lax.axis_index("tm")
    i = lax.axis_index("space")
    after, before = lax.rem(t + 1, n_tm), lax.rem(t + n_tm - 1, n_tm)
    above, below = lax.rem(i + 1, n_space), lax.rem(i + n_space - 1, n_space)

    fetches = [
        pltpu.make_async_copy(gauge_hbm, gauge_in, local_sem.at[0]),
        pltpu.make_async_copy(temporal_hbm, temporal_in, local_sem.at[1]),
        pltpu.make_async_copy(sinks_hbm, sinks, local_sem.at[2]),
    ]
    for fetch in fetches:
        fetch.start()

    barrier = pltpu.get_barrier_semaphore()
    for near_t in (before, after):
        for near_i in (below, i, above):
            pl.semaphore_signal(
                barrier, inc=1, device_id={"tm": near_t, "space": near_i}, device_id_type=MESH
            )
    for step in range(1, n_space):
        pl.semaphore_signal(
            barrier, inc=1,
            device_id={"tm": t, "space": lax.rem(i + step, n_space)}, device_id_type=MESH,
        )

    recv_own[0] = jnp.zeros_like(recv_own[0])
    recv_low[0] = jnp.zeros_like(recv_low[0])
    recv_high[0] = jnp.zeros_like(recv_high[0])

    start = [times_ref[k] for k in range(SLOTS)]
    late, lane = schedule(start, n_tm)
    here, which = [], []
    for d in range(SLOTS):
        count = jnp.int32(0)
        index = [jnp.int32(0), jnp.int32(0)]
        for k in range(SLOTS):
            match = jnp.where(start[k] == t, jnp.where(late[k] == d, 1, 0), 0)
            count = count + match
            index = [index[j] + match * index_ref[j, k] for j in range(2)]
        here.append(count)
        which.append(index)

    fetches[0].wait()
    fetches[1].wait()
    for x in range(2):
        for row in range(3):
            for col in range(3):
                for mu in range(4):
                    pair = []
                    for ri in range(2):
                        if mu == 3:
                            plane = temporal_in[ri, row, col, pl.ds(x, 8, stride=2), :]
                            link_t[1 + x, ri, row, col] = plane
                        else:
                            plane = gauge_in[ri, mu, row, col, pl.ds(x, 8, stride=2), :]
                            if mu == 0:
                                link_x[2 + x, ri, row, col] = plane
                            else:
                                link_yz[1 + x, mu - 1, ri, row, col] = plane
                        pair.append(plane)
                    if row < 2:
                        packed = jnp.concatenate(pair, axis=0).astype(BF16)
                        if x == 1:
                            up_out[mu, row * 3 + col] = packed
                        else:
                            down_out[mu, row * 3 + col] = packed
                            if mu == 0:
                                up_out[4, row * 3 + col] = packed

    pl.semaphore_wait(barrier, 6 + n_space - 1)

    def halo(number, src, dst, device):
        return pltpu.make_async_remote_copy(
            src_ref=src, dst_ref=dst, send_sem=halo_send.at[number], recv_sem=halo_recv.at[number],
            device_id={"tm": t, "space": device}, device_id_type=MESH,
        )

    link_halos = (
        halo(2 * SLOTS, up_out, low_links, above),
        halo(2 * SLOTS + 1, down_out, high_links, below),
    )
    for copy in link_halos:
        copy.start()

    fetches[2].wait()
    source_halos = []
    for d in range(slots):
        keep = here[d].astype(F32)
        for j in range(2):
            for ri in range(2):
                for c in range(3):
                    staged[d, j, ri * 3 + c] = sinks[ri, which[d][j], c].astype(F32) * keep
            for part in range(6):
                planes = [staged[d, j, part, pl.ds(x, 8, stride=2), :] for x in range(2)]
                own_src[d, j, part] = jnp.concatenate(planes, axis=0).astype(BF16)
        source_halos.append(
            (
                halo(2 * d, own_src.at[d], low_src.at[d], above),
                halo(2 * d + 1, own_src.at[d], high_src.at[d], below),
            )
        )
        for copy in source_halos[d]:
            copy.start()

    def unpack(packed, store):
        rows = [[packed[row * 3 + col].astype(F32) for col in range(3)] for row in range(2)]
        re = [[entry[0:8] for entry in row] for row in rows]
        im = [[entry[8:16] for entry in row] for row in rows]
        last_re, last_im = [], []
        for col in range(3):
            a, b = (col + 1) % 3, (col + 2) % 3
            last_re.append(
                (re[0][a] * re[1][b] - im[0][a] * im[1][b]) - (re[0][b] * re[1][a] - im[0][b] * im[1][a])
            )
            last_im.append(
                (re[0][b] * im[1][a] + im[0][b] * re[1][a]) - (re[0][a] * im[1][b] + im[0][a] * re[1][b])
            )
        re, im = re + [last_re], im + [last_im]
        for row in range(3):
            for col in range(3):
                store[0, row, col] = re[row][col]
                store[1, row, col] = im[row][col]

    for arrived, copy, x_plane, plane in (
        (high_links, link_halos[1], 4, 3),
        (low_links, link_halos[0], 1, 0),
    ):
        copy.wait_recv()
        unpack(arrived.at[0], link_x.at[x_plane])
        unpack(arrived.at[1], link_yz.at[plane, 0])
        unpack(arrived.at[2], link_yz.at[plane, 1])
        unpack(arrived.at[3], link_t.at[plane])
    unpack(low_links.at[4], link_x.at[0])

    lanes = lax.broadcasted_iota(jnp.int32, (3, 8, 128), 2)
    z = lax.rem(lanes, 32)
    first_z, last_z = z == 0, z == 31
    low_lanes, high_lanes = lanes < 32, lanes >= 96

    def up(values, direction):
        if direction == 0:
            moved = pltpu.roll(values, 96, 2)
            return jnp.where(high_lanes, pltpu.roll(moved, 7, 1), moved)
        return jnp.where(last_z, pltpu.roll(values, 31, 2), pltpu.roll(values, 127, 2))

    def down(values, direction):
        if direction == 0:
            moved = pltpu.roll(values, 32, 2)
            return jnp.where(low_lanes, pltpu.roll(moved, 1, 1), moved)
        return jnp.where(first_z, pltpu.roll(values, 97, 2), pltpu.roll(values, 1, 2))

    def neighbours(source, q, links_q, total=None, x_up=True, x_down=True, flat=True):
        at = lambda p: (source[p, 0:3], source[p, 3:6])

        def plus(more):
            return more if total is None else (total[0] + more[0], total[1] + more[1])

        if flat:
            centre = at(q)
            for direction in range(2):
                links = lambda ri, a, b: link_yz[links_q, direction, ri, a, b]
                total = plus(times(links, tuple(up(part, direction) for part in centre)))
                total = plus(tuple(down(part, direction) for part in adjoint_times(links, centre)))
        if x_up:
            total = plus(times(lambda ri, a, b: link_x[links_q + 1, ri, a, b], at(q + 1)))
        if x_down:
            total = plus(adjoint_times(lambda ri, a, b: link_x[links_q, ri, a, b], at(q - 1)))
        return total

    def relaxed(source, q, total, weight):
        rest = 1.0 - 6.0 * weight
        return rest * source[q, 0:3] + weight * total[0], rest * source[q, 3:6] + weight * total[1]

    def hop(number, device_t, r, j):
        if number == 0:
            src, dst, target = record.at[r, j], recv_low.at[r + 1, j], above
        elif number == 1:
            src, dst, target = record.at[r, j], recv_high.at[r + 1, j], below
        else:
            src, dst, target = sent_own.at[r, j], recv_own.at[r + 1, j], i
        return pltpu.make_async_remote_copy(
            src_ref=src, dst_ref=dst,
            send_sem=step_send.at[r, j, number], recv_sem=step_recv.at[r, j, number],
            device_id={"tm": device_t, "space": target}, device_id_type=MESH,
        )

    def one_source(n, carry):
        r, j = n // 2, lax.rem(n, 2)
        d = jnp.minimum(r, slots - 1)
        take = jnp.where(r == 0, 1, 0)
        for late_by in range(1, slots):
            take = jnp.where(r == late_by, here[late_by], take)

        @pl.when(r > 0)
        def _():
            hop(2, after, r - 1, j).wait_recv()

        @pl.when(r < slots)
        def _():
            inject = jnp.full((16, 128), take, jnp.int32) > 0
            for part in range(6):
                arrived = jnp.concatenate([recv_own[r, j, x, part] for x in range(2)], axis=0)
                value = jnp.where(inject, own_src[d, j, part].astype(F32), arrived)
                field[2, part] = value[0:8]
                field[3, part] = value[8:16]

        @pl.when(r >= slots)
        def _():
            for part in range(6):
                for x in range(2):
                    field[2 + x, part] = recv_own[r, j, x, part]

        for q in (1, 2):
            re, im = neighbours(field, q + 1, q, x_up=q == 1, x_down=q == 2)
            early[q - 1, 0:3] = re
            early[q - 1, 3:6] = im

        on_lane = lax.rem(t - r + 2 * n_tm, n_tm)
        weight = jnp.float32(0)
        for k in range(SLOTS):
            weight = jnp.where(lane[k] == on_lane, 0.5 * coef_ref[j, k], weight)

        for side, place, begun, came, planes in (
            (0, 0, low_src, recv_low, (0, 1)),
            (1, 4, high_src, recv_high, (3, 2)),
        ):
            for late_by in range(slots):

                @pl.when(n == 2 * late_by)
                def _():
                    source_halos[late_by][side].wait_recv()

            @pl.when(r > 0)
            def _():
                hop(side, after, r - 1, j).wait_recv()

            @pl.when(r < slots)
            def _():
                inject = jnp.full((16, 128), take, jnp.int32) > 0
                for part in range(6):
                    value = jnp.where(inject, begun[d, j, part], came[r, j, part]).astype(F32)
                    field[place, part] = value[0:8]
                    field[place + 1, part] = value[8:16]

            @pl.when(r >= slots)
            def _():
                for part in range(6):
                    value = came[r, j, part].astype(F32)
                    field[place, part] = value[0:8]
                    field[place + 1, part] = value[8:16]

            for q in planes:
                if q == 0 or q == 3:
                    total = neighbours(field, q + 1, q)
                else:
                    total = neighbours(
                        field, q + 1, q, (early[q - 1, 0:3], early[q - 1, 3:6]),
                        x_up=q == 2, x_down=q == 1, flat=False,
                    )
                half = relaxed(field, q + 1, total, weight)
                re, im = adjoint_times(lambda ri, a, b: link_t[q, ri, a, b], half)
                turned[q, 0:3] = re
                turned[q, 3:6] = im
        results = []
        for x in range(2):
            re, im = relaxed(turned, x + 1, neighbours(turned, x + 1, x + 1), weight)
            sent_own[r, j, x, 0:3] = re
            sent_own[r, j, x, 3:6] = im
            results.append((re, im))
        for ri in range(2):
            both = jnp.concatenate([results[0][ri], results[1][ri]], axis=1)
            record[r, j, 3 * ri : 3 * ri + 3] = both.astype(BF16)

        @pl.when(r < rounds - 1)
        def _():
            for number in range(3):
                hop(number, after, r, j).start()

        return carry

    lax.fori_loop(0, 2 * rounds, one_source, 0)

    for k in range(SLOTS):
        round_of = jnp.minimum(late[k] + modulo(t - start[k], n_tm), rounds - 1)
        for j in range(2):
            for c in range(3):
                spot = (k * 2 + j) * 16
                re, im = record[round_of, j, c], record[round_of, j, 3 + c]
                chosen[c, spot : spot + 16] = jnp.concatenate([re, im], axis=1)
                chosen[c, 128 + spot : 128 + spot + 16] = jnp.concatenate([im, -re], axis=1)
    row = lax.broadcasted_iota(jnp.int32, (16, 256), 0)
    col = lax.rem(lax.broadcasted_iota(jnp.int32, (16, 256), 1), 16)
    same = jnp.where(row == 2 * lax.rem(col, 8) + col // 8, 1.0, 0.0).astype(F32)
    n_sinks = sinks.shape[1]

    def some_sinks(step, carry):
        first = pl.multiple_of(step * 64, 64)
        products = None
        for c in range(3):
            block = jnp.concatenate([sinks[ri, pl.ds(first, 64), c].reshape(1024, 128) for ri in range(2)], axis=1)
            product = lax.dot_general(
                block, chosen[c], (((1,), (1,)), ((), ())), preferred_element_type=F32
            )
            products = product if products is None else products + product
        products = products.reshape(64, 16, 256) * same[None]
        summed[pl.ds(first, 64), :] = jnp.sum(products, axis=1)
        return carry

    lax.fori_loop(0, n_sinks // 64, some_sinks, 0, unroll=False)
    entry = lax.broadcasted_iota(jnp.int32, (256, 128), 0) // 16
    column = lax.broadcasted_iota(jnp.int32, (256, 128), 1)
    fold = jnp.where(entry == column, 1.0, 0.0).astype(F32)
    partial[...] = jnp.dot(
        summed[...], fold, precision=lax.Precision.HIGHEST, preferred_element_type=F32
    )

    share = n_sinks // n_space

    def give(step):
        target = lax.rem(i + step, n_space)
        return pltpu.make_async_remote_copy(
            src_ref=partial.at[pl.ds(pl.multiple_of(target * share, share), share)],
            dst_ref=parts.at[step],
            send_sem=part_send.at[step], recv_sem=part_recv.at[step],
            device_id={"tm": t, "space": target}, device_id_type=MESH,
        )

    for step in range(1, n_space):
        give(step).start()
    total = partial[pl.ds(pl.multiple_of(i * share, share), share), :]
    for step in range(1, n_space):
        give(step).wait_recv()
        total = total + parts[step]
    out_ref[...] = total

    for step in range(1, n_space):
        give(step).wait_send()
    for copy in sum(source_halos, link_halos):
        copy.wait_send()

    def finish(n, carry):
        for number in range(3):
            hop(number, after, n // 2, lax.rem(n, 2)).wait_send()
        return carry

    lax.fori_loop(0, 2 * (rounds - 1), finish, 0)


def latest_start(n_tm, times_ref, out_ref):
    late, _ = schedule([times_ref[k] for k in range(SLOTS)], n_tm)
    latest = late[0]
    for d in late[1:]:
        latest = jnp.maximum(latest, d)
    out_ref[0] = latest


def rows_of(x):
    lead = x.shape[:-2]
    x = x.reshape(*lead, 2, 8, 128)
    x = jnp.swapaxes(x, x.ndim - 3, x.ndim - 2)
    return x.reshape(*lead, 16, 128)


def local(gauge_links, time_links, sink_vectors, source_times, source_index, kinetic_coef):
    n_tm, n_space = lax.axis_size("tm"), lax.axis_size("space")
    n_sinks = sink_vectors.shape[2]
    share = n_sinks // n_space
    smem = pl.BlockSpec(memory_space=pltpu.SMEM)
    hbm = pl.BlockSpec(memory_space=pl.ANY)
    vmem = pltpu.VMEM
    dma = pltpu.SemaphoreType.DMA

    def with_slots(slots):
        rounds = n_tm + slots - 1
        return pl.pallas_call(
            functools.partial(kernel, n_tm, n_space, slots),
            out_shape=jax.ShapeDtypeStruct((share, 128), F32),
            in_specs=[smem, smem, smem, hbm, hbm, hbm],
            out_specs=pl.BlockSpec(memory_space=pltpu.VMEM),
            scratch_shapes=[
                vmem((2, 3, 3, 3, 16, 128), F32),
                vmem((2, 3, 3, 16, 128), F32),
                vmem((2, n_sinks, 3, 16, 128), BF16),
                vmem((5, 2, 3, 3, 8, 128), F32),
                vmem((4, 2, 2, 3, 3, 8, 128), F32),
                vmem((4, 2, 3, 3, 8, 128), F32),
                vmem((5, 6, 16, 128), BF16),
                vmem((4, 6, 16, 128), BF16),
                vmem((5, 6, 16, 128), BF16),
                vmem((4, 6, 16, 128), BF16),
                vmem((slots, 2, 6, 16, 128), F32),
                vmem((slots, 2, 6, 16, 128), BF16),
                vmem((slots, 2, 6, 16, 128), BF16),
                vmem((slots, 2, 6, 16, 128), BF16),
                vmem((rounds, 2, 2, 6, 8, 128), F32),
                vmem((rounds, 2, 6, 16, 128), BF16),
                vmem((rounds, 2, 6, 16, 128), BF16),
                vmem((rounds, 2, 2, 6, 8, 128), F32),
                vmem((rounds, 2, 6, 16, 128), BF16),
                vmem((6, 6, 8, 128), F32),
                vmem((2, 6, 8, 128), F32),
                vmem((4, 6, 8, 128), F32),
                vmem((3, 256, 256), BF16),
                vmem((n_sinks, 256), F32),
                vmem((n_sinks, 128), F32),
                vmem((n_space, share, 128), F32),
                dma((3,)),
                dma((2 * SLOTS + 2,)),
                dma((2 * SLOTS + 2,)),
                dma((rounds - 1, 2, 3)),
                dma((rounds - 1, 2, 3)),
                dma((n_space,)),
                dma((n_space,)),
            ],
            compiler_params=pltpu.CompilerParams(collective_id=slots - 1, has_side_effects=True),
        )

    latest = pl.pallas_call(
        functools.partial(latest_start, n_tm),
        out_shape=jax.ShapeDtypeStruct((1,), jnp.int32),
        in_specs=[smem],
        out_specs=smem,
    )(source_times)[0]
    result = lax.switch(
        latest,
        [with_slots(slots) for slots in range(1, SLOTS + 1)],
        source_times, source_index.T, kinetic_coef.T,
        rows_of(gauge_links[0]), rows_of(time_links[0]), rows_of(sink_vectors[0]),
    )
    groups, per_group = kinetic_coef.shape
    table = result[:, : 2 * groups * per_group].reshape(share, 2, groups, per_group)
    return jnp.moveaxis(table, 0, 3)[:, :, :, None, :]


def solution(mesh):
    placed = (
        P("tm", None, None, None, None, "space", None),
        P("tm", None, None, None, "space", None),
        P("tm", None, None, None, "space", None),
        P(),
        P(),
        P(),
    )
    return jax.shard_map(
        local,
        mesh=mesh,
        in_specs=placed,
        out_specs=P(None, None, None, "tm", "space"),
        check_vma=False,
    )
```
